32 devices in a mesh: dp: 8 (over z, x), tensor: 4 (over y, core).
Axes of the slice: x: 2, y: 2, z: 4, core: 2. Of those that a mesh axis runs over, the one named last changes fastest.
Arguments:
- lang_in: bfloat16 [3840, 768], P(('dp', 'tensor')), may hold values from -6 to 6
- visn_in: bfloat16 [6912, 768], P(('dp', 'tensor')), may hold values from -6 to 6
- word_mask: int32 [192, 20], P('dp'), may hold values from 0 to 1, as said below
- task_flag: int32 [192], P('dp'), may hold values from 0 to 2
- group_id: int32 [192], P('dp'), may hold values from 0 to 4
- task_table: bfloat16 [3, 768], replicated, may hold values from -3 to 3
- group_table: bfloat16 [5, 768], replicated, may hold values from -3 to 3
- attn_in: bfloat16 [3, 3, 768, 768], P(None, None, None, 'tensor'), may hold values from -0.21875 to 0.21875
- attn_qv_bias: bfloat16 [3, 2, 768], P(None, None, 'tensor'), may hold values from -3 to 3
- attn_out: bfloat16 [3, 768, 768], P(None, 'tensor'), may hold values from -0.625 to 0.625
- ffn_in: bfloat16 [2, 768, 3072], P(None, None, 'tensor'), may hold values from -0.21875 to 0.21875
- ffn_in_bias: bfloat16 [2, 3072], P(None, 'tensor'), may hold values from -3 to 3
- ffn_out: bfloat16 [2, 3072, 768], P(None, 'tensor'), may hold values from -0.15625 to 0.15625
- out_bias: bfloat16 [5, 768], replicated, may hold values from -2 to 2
- norm_gain: bfloat16 [5, 768], replicated, may hold values from 0.099609375 to 1.8984375
- norm_bias: bfloat16 [5, 768], replicated, may hold values from -2 to 2
- lang_cot: bfloat16 [3840, 768], P(('dp', 'tensor')), may hold values from -6 to 6
- visn_cot: bfloat16 [6912, 768], P(('dp', 'tensor')), may hold values from -6 to 6
Outputs:
- lang_out: bfloat16 [3840, 768], P(('dp', 'tensor'))
- visn_out: bfloat16 [6912, 768], P(('dp', 'tensor'))
- lang_grad: bfloat16 [3840, 768], P(('dp', 'tensor'))
- visn_grad: bfloat16 [6912, 768], P(('dp', 'tensor'))
- task_grad: float32 [3, 768], replicated
- group_grad: float32 [5, 768], replicated
- attn_in_grad: float32 [3, 3, 768, 768], P(None, None, 'dp', 'tensor')
- qv_bias_grad: float32 [3, 2, 768], P(None, None, 'tensor')
- attn_out_grad: float32 [3, 768, 768], P(None, 'tensor', 'dp')
- ffn_in_grad: float32 [2, 768, 3072], P(None, 'dp', 'tensor')
- ffn_bias_grad: float32 [2, 3072], P(None, 'tensor')
- ffn_out_grad: float32 [2, 3072, 768], P(None, 'tensor', 'dp')
- out_bias_grad: float32 [5, 768], replicated
- gain_grad: float32 [5, 768], replicated
- shift_grad: float32 [5, 768], replicated
The draws below stay inside these ranges and needn't reach their ends.
Inputs may be any that keep to these rules, and one draw needn't show every extreme that they name: `word_mask`: each item's mask is 1 on its first 6 to 20 word slots and 0 after them.
All inputs are finite; a program needn't handle non-finite values.
Results may differ from the reference program's by a relative error of at most 0.035.
Values may be sent and summed in bfloat16 or wider, within the bound.
A program may use at most 192 MiB of HBM per device.

```python
import jax
import jax.numpy as jnp
from jax import lax

D = 768
HEADS = 12
HEAD = 64
FF = 3072
WORDS = 20
REGIONS = 36
TASKS = 3
GROUPS = 5
ITEMS_DEV = 24
ITEMS = 192
N_DP = 8


def draw_word_mask(key, part):
    length = jax.random.randint(key, (ITEMS, 1), 6, WORDS + 1)
    return (jnp.arange(WORDS, dtype=jnp.int32)[None, :] < length).astype(jnp.int32)


def with_ends(entries, rng, smallest, top_value):
    shape = entries.shape
    place = [jax.random.randint(jax.random.fold_in(rng, axis), (), 0, shape[axis]) for axis in range(len(shape))]
    entries = entries.at[tuple(place)].set(smallest)
    longest = shape.index(max(shape))
    place[longest] = (place[longest] + 1) % shape[longest]
    return entries.at[tuple(place)].set(top_value)


def raised(array, own_key, source, target, parts, factor):
    owner, partner = [(jnp.arange(array.shape[axis_at]) // (array.shape[axis_at] // parts)).reshape([-1 if axis == axis_at else 1 for axis in range(array.ndim)]) for axis_at in (source, target)]
    chosen = jax.random.permutation(own_key, parts)[partner]
    strong = (owner == chosen) | (owner == (partner + parts // 2) % parts)
    return jnp.where(strong, factor * array, array)


def block_scale(key, shape, cuts, low, high):
    def one(dim, shards_of):
        steps = jax.random.uniform(jax.random.fold_in(jax.random.fold_in(key, 6), dim), (shards_of,), jnp.float32, low / len(cuts), high / len(cuts))
        return jnp.repeat(jnp.exp(steps), shape[dim] // shards_of).reshape((-1,) + (1,) * (len(shape) - dim - 1))

    level = one(*cuts[0])
    for cut in cuts[1:]:
        level = level * one(*cut)
    return level


def scatter_about(own_key, extent, width, most, cuts=(), held_as=jnp.bfloat16):
    drawn = jax.random.normal(own_key, extent, jnp.float32) * width
    if len(cuts) > 0:
        drawn = block_scale(own_key, extent, cuts, -0.22, 0.18) * drawn
    return jnp.clip(drawn, min=-most, max=most).astype(held_as)


def bell_draw_with(key, shape, scale, most, shards, heavy, kind=jnp.bfloat16):
    result = scale * jax.random.normal(key, shape, jnp.float32)
    if shards:
        result = result * block_scale(key, shape, shards, -0.22, 0.18)
    return jnp.clip(raised(result, jax.random.fold_in(key, 3), *heavy), -most, most).astype(kind)


def setup_inputs(seed: int = 0) -> dict:
    key_list = jax.random.split(jax.random.key(seed), 19)
    lang_in = bell_draw_with(key_list[0], (ITEMS * WORDS, D), 1.0, 6.0, ((0, 32),), (0, 1, 32, 2.75))
    visn_in = bell_draw_with(key_list[1], (ITEMS * REGIONS, D), 1.0, 6.0, ((0, 32),), (0, 1, 32, 2.75))
    word_mask = draw_word_mask(jax.random.fold_in(key_list[18], 71), 0)
    task_flag = with_ends(jax.random.randint(key_list[3], (ITEMS,), 0, TASKS), jax.random.fold_in(key_list[3], 1), 0, TASKS - 1).astype(jnp.int32)
    group_id = with_ends(jax.random.randint(key_list[4], (ITEMS,), 0, GROUPS), jax.random.fold_in(key_list[4], 1), 0, GROUPS - 1).astype(jnp.int32)
    task_table = scatter_about(key_list[5], (TASKS, D), 0.5, 3.0)
    group_table = scatter_about(key_list[6], (GROUPS, D), 0.5, 3.0)
    attn_in = scatter_about(key_list[7], (3, 3, D, D), D ** -0.5, 0.21875, ((3, 4),))
    attn_qv_bias = scatter_about(key_list[8], (3, 2, D), 0.5, 3.0, ((2, 4),))
    attn_out = scatter_about(key_list[9], (3, D, D), (D // 8) ** -0.5, 0.625, ((1, 4),))
    ffn_in = scatter_about(key_list[10], (2, D, FF), D ** -0.5, 0.21875, ((2, 4),))
    ffn_in_bias = scatter_about(key_list[11], (2, FF), 0.5, 3.0, ((1, 4),))
    ffn_out = scatter_about(key_list[12], (2, FF, D), (FF // 2) ** -0.5, 0.15625, ((1, 4),))
    out_bias = scatter_about(key_list[13], (5, D), 0.3, 2.0)
    norm_gain = jnp.clip(1.0 + 0.18 * jax.random.normal(key_list[14], (5, D), jnp.float32), 0.099609375, 1.8984375).astype(jnp.bfloat16)
    norm_bias = scatter_about(key_list[15], (5, D), 0.3, 2.0)
    lang_cot = bell_draw_with(key_list[16], (ITEMS * WORDS, D), 1.0, 6.0, ((0, 32),), (0, 1, 32, 2.75))
    visn_cot = bell_draw_with(key_list[17], (ITEMS * REGIONS, D), 1.0, 6.0, ((0, 32),), (0, 1, 32, 2.75))
    return {"lang_in": lang_in, "visn_in": visn_in, "word_mask": word_mask, "task_flag": task_flag, "group_id": group_id, "task_table": task_table, "group_table": group_table, "attn_in": attn_in, "attn_qv_bias": attn_qv_bias, "attn_out": attn_out, "ffn_in": ffn_in, "ffn_in_bias": ffn_in_bias, "ffn_out": ffn_out, "out_bias": out_bias, "norm_gain": norm_gain, "norm_bias": norm_bias, "lang_cot": lang_cot, "visn_cot": visn_cot}


@jax.custom_vjp
def low(v):
    return lax.optimization_barrier(v.astype(jnp.bfloat16)).astype(jnp.float32)

@jax.custom_vjp
def low_back(v):
    return v

def low_keep(v):
    return (low(v), None)

def low_pass(kept, grad):
    return (grad,)

def back_keep(v):
    return (v, None)

def back_low(kept, grad):
    return (low(grad),)
low.defvjp(low_keep, low_pass)
low_back.defvjp(back_keep, back_low)
norm_eps = 1e-06
root_half = 0.7071067811865476
highest = lax.Precision.HIGHEST

def layer_norm(pre_norm, gain_vec, shift_vec):
    average = lax.optimization_barrier(jnp.mean(pre_norm, axis=-1, keepdims=True))
    centred = pre_norm - average
    spread = lax.optimization_barrier(jnp.mean(centred * centred, axis=-1, keepdims=True))
    return centred * lax.rsqrt(spread + norm_eps) * gain_vec + shift_vec

def project(source, weight):
    return jnp.einsum('bnd,de->bne', source, weight, precision=highest)

def split_heads(flattened):
    return flattened.reshape(flattened.shape[0], flattened.shape[1], HEADS, HEAD)

def attention(source_q, source_kv, keep_mask, weights, biases, w_out):
    queries = low(low_back(project(source_q, weights[0]) + biases[0]))
    key_rows = low(low_back(project(source_kv, weights[1])))
    values = low(low_back(project(source_kv, weights[2]) + biases[1]))
    raw_scores = jnp.einsum('bqhd,bkhd->bhqk', split_heads(queries), split_heads(key_rows), precision=highest) * HEAD ** (-0.5)
    scores = low_back(jnp.where(keep_mask[:, None, None, :], raw_scores, -1000000000.0))
    row_max = lax.optimization_barrier(jnp.max(scores, axis=-1, keepdims=True))
    powers = jnp.exp(scores - row_max)
    attn_probs = low(powers / lax.optimization_barrier(jnp.sum(powers, axis=-1, keepdims=True)))
    context = jnp.einsum('bhqk,bkhd->bqhd', attn_probs, split_heads(values), precision=highest)
    context = low(low_back(context.reshape(queries.shape)))
    return low_back(project(context, w_out))

def gelu_value(pre_act):
    return 0.5 * pre_act * (1.0 + lax.erf(pre_act * root_half))

def feed_forward(source, w_in, b_in, w_out):
    hidden = low_back(project(low(source), w_in) + b_in)
    active = low(gelu_value(hidden))
    return low_back(project(active, w_out))

def forward(lang_now, visn_now, keep_mask, task_hot, group_hot, params):
    task_table, group_table, attn_in, qv_bias, attn_out, ffn_in, ffn_bias, ffn_out, out_bias, gains, shifts = params
    lang_base = lang_now + jnp.dot(task_hot, task_table, precision=highest, preferred_element_type=jnp.float32)[:, None, :]
    visn_base = visn_now + jnp.dot(group_hot, group_table, precision=highest, preferred_element_type=jnp.float32)[:, None, :]
    lang_low = low(lang_base)
    visn_low = low(visn_base)
    every_region = jnp.ones(visn_now.shape[:2], dtype=jnp.bool_)
    cross_lang = attention(lang_low, visn_low, every_region, attn_in[0], qv_bias[0], attn_out[0])
    cross_visn = attention(visn_low, lang_low, keep_mask, attn_in[0], qv_bias[0], attn_out[0])
    lang_one = layer_norm(lang_base + cross_lang + out_bias[0], gains[0], shifts[0])
    visn_one = layer_norm(visn_base + cross_visn + out_bias[0], gains[0], shifts[0])
    lang_src = low(lang_one)
    lang_two = layer_norm(lang_one + attention(lang_src, lang_src, keep_mask, attn_in[1], qv_bias[1], attn_out[1]) + out_bias[1], gains[1], shifts[1])
    visn_src = low(visn_one)
    visn_two = layer_norm(visn_one + attention(visn_src, visn_src, every_region, attn_in[2], qv_bias[2], attn_out[2]) + out_bias[2], gains[2], shifts[2])
    lang_out = layer_norm(lang_two + feed_forward(lang_two, ffn_in[0], ffn_bias[0], ffn_out[0]) + out_bias[3], gains[3], shifts[3])
    visn_out = layer_norm(visn_two + feed_forward(visn_two, ffn_in[1], ffn_bias[1], ffn_out[1]) + out_bias[4], gains[4], shifts[4])
    return (lang_out, visn_out)

def reference(lang_in, visn_in, word_mask, task_flag, group_id, task_table, group_table, attn_in, attn_qv_bias, attn_out, ffn_in, ffn_in_bias, ffn_out, out_bias, norm_gain, norm_bias, lang_cot, visn_cot):
    params = tuple((member.astype(jnp.float32) for member in (task_table, group_table, attn_in, attn_qv_bias, attn_out, ffn_in, ffn_in_bias, ffn_out, out_bias, norm_gain, norm_bias)))
    lang_blocks = lang_in.reshape(N_DP, ITEMS_DEV, WORDS, D)
    visn_blocks = visn_in.reshape(N_DP, ITEMS_DEV, REGIONS, D)
    lcot_blocks = lang_cot.reshape(N_DP, ITEMS_DEV, WORDS, D)
    vcot_blocks = visn_cot.reshape(N_DP, ITEMS_DEV, REGIONS, D)
    keep_blocks = (word_mask > 0).reshape(N_DP, ITEMS_DEV, WORDS)
    task_hot = (task_flag[:, None] == jnp.arange(TASKS, dtype=jnp.int32)[None, :]).astype(jnp.float32).reshape(N_DP, ITEMS_DEV, TASKS)
    group_hot = (group_id[:, None] == jnp.arange(GROUPS, dtype=jnp.int32)[None, :]).astype(jnp.float32).reshape(N_DP, ITEMS_DEV, GROUPS)

    def one_block(totals, inputs):
        lang_part, visn_part, keep_part, task_part, group_part, lcot_part, vcot_part = inputs

        def run_layer(lang_now, visn_now, *weights):
            return forward(lang_now, visn_now, keep_part, task_part, group_part, weights)
        outputs, pull_back = jax.vjp(run_layer, lang_part.astype(jnp.float32), visn_part.astype(jnp.float32), *params)
        grad_list = pull_back((lcot_part.astype(jnp.float32), vcot_part.astype(jnp.float32)))
        totals = tuple((summed + grad_term for summed, grad_term in zip(totals, grad_list[2:])))
        return (totals, (outputs[0].astype(jnp.bfloat16), outputs[1].astype(jnp.bfloat16), grad_list[0].astype(jnp.bfloat16), grad_list[1].astype(jnp.bfloat16)))
    zero_grads = tuple((jnp.zeros(member.shape, jnp.float32) for member in params))
    totals, stacked = lax.scan(one_block, zero_grads, (lang_blocks, visn_blocks, keep_blocks, task_hot, group_hot, lcot_blocks, vcot_blocks))
    task_grad, group_grad, attn_in_grad, qv_bias_grad, attn_out_grad, ffn_in_grad, ffn_bias_grad, ffn_out_grad, out_bias_grad, gain_grad, shift_grad = totals
    lang_out = stacked[0].reshape(ITEMS * WORDS, D)
    visn_out = stacked[1].reshape(ITEMS * REGIONS, D)
    lang_grad = stacked[2].reshape(ITEMS * WORDS, D)
    visn_grad = stacked[3].reshape(ITEMS * REGIONS, D)
    return (lang_out, visn_out, lang_grad, visn_grad, task_grad, group_grad, attn_in_grad, qv_bias_grad, attn_out_grad, ffn_in_grad, ffn_bias_grad, ffn_out_grad, out_bias_grad, gain_grad, shift_grad)
```

```python
import functools

import jax
import jax.numpy as jnp
from jax import lax
from jax.experimental import pallas as pl
from jax.experimental.pallas import tpu as pltpu
from jax.sharding import PartitionSpec as P

HEAD = 64
WORDS = 20
REGIONS = 36
TASKS = 3
GROUPS = 5


norm_eps = 1e-06
root_half = 0.7071067811865476
inv_root_tau = 0.3989422804014327
highest = lax.Precision.HIGHEST


def linear(source, weight):
    return jnp.dot(source, weight, preferred_element_type=jnp.float32)


def linear_back(upstream, weight):
    return lax.dot_general(
        upstream, weight, (((1,), (1,)), ((), ())), preferred_element_type=jnp.float32
    )


def weight_grad(source, upstream):
    return lax.dot_general(
        source, upstream, (((0,), (0,)), ((), ())), preferred_element_type=jnp.float32
    )


def column_sum(upstream):
    return jnp.sum(upstream.astype(jnp.float32), axis=0)


def gelu_value(pre_act):
    return 0.5 * pre_act * (1.0 + lax.erf(pre_act * root_half))


def gelu_slope(pre_act):
    return (
        0.5 * (1.0 + lax.erf(pre_act * root_half))
        + pre_act * jnp.exp(-0.5 * pre_act * pre_act) * inv_root_tau
    )


def norm_forward(pre_norm, gain_vec, shift_vec):
    average = jnp.mean(pre_norm, axis=-1, keepdims=True)
    centred = pre_norm - average
    spread = jnp.mean(centred * centred, axis=-1, keepdims=True)
    inverse = lax.rsqrt(spread + norm_eps)
    normed = centred * inverse
    return (normed * gain_vec + shift_vec, (normed, inverse))


def norm_backward(out_grad, stash, gain_vec):
    normed, inverse = stash
    scaled = out_grad * gain_vec
    in_grad = inverse * (
        scaled
        - jnp.mean(scaled, axis=-1, keepdims=True)
        - normed * jnp.mean(scaled * normed, axis=-1, keepdims=True)
    )
    return (
        in_grad,
        jnp.sum(out_grad * normed, axis=0),
        jnp.sum(out_grad, axis=0),
        jnp.sum(in_grad, axis=0),
    )


def split_heads(flattened, item_count):
    return flattened.reshape(
        item_count, flattened.shape[0] // item_count, flattened.shape[1] // HEAD, HEAD
    )


def merge_heads(split_rows):
    return split_rows.reshape(
        split_rows.shape[0] * split_rows.shape[1], split_rows.shape[2] * split_rows.shape[3]
    )


def attend_forward(source_q, source_kv, keep_mask, weights, biases, item_count):
    queries = (linear(source_q, weights[0]) + biases[0]).astype(jnp.bfloat16)
    key_rows = linear(source_kv, weights[1]).astype(jnp.bfloat16)
    values = (linear(source_kv, weights[2]) + biases[1]).astype(jnp.bfloat16)
    score_scale = HEAD ** (-0.5)
    scores = (
        jnp.einsum(
            "bqhd,bkhd->bhqk",
            split_heads(queries, item_count),
            split_heads(key_rows, item_count),
            preferred_element_type=jnp.float32,
        )
        * score_scale
    )
    if keep_mask is not None:
        scores = jnp.where(keep_mask[:, None, None, :], scores, -1000000000.0)
    row_max = jnp.max(scores, axis=-1, keepdims=True)
    powers = jnp.exp(scores - row_max)
    attn_probs = powers / jnp.sum(powers, axis=-1, keepdims=True)
    probs_low = attn_probs.astype(jnp.bfloat16)
    context = jnp.einsum(
        "bhqk,bkhd->bqhd",
        probs_low,
        split_heads(values, item_count),
        preferred_element_type=jnp.float32,
    )
    context = merge_heads(context).astype(jnp.bfloat16)
    return (context, (queries, key_rows, values, attn_probs, probs_low))


def attend_backward(grad_context, stash, item_count):
    queries, key_rows, values, attn_probs, probs_low = stash
    score_scale = HEAD ** (-0.5)
    grad_heads = split_heads(grad_context.astype(jnp.bfloat16), item_count)
    grad_probs = jnp.einsum(
        "bqhd,bkhd->bhqk",
        grad_heads,
        split_heads(values, item_count),
        preferred_element_type=jnp.float32,
    )
    grad_values = jnp.einsum(
        "bhqk,bqhd->bkhd", probs_low, grad_heads, preferred_element_type=jnp.float32
    )
    grad_scores = attn_probs * (
        grad_probs - jnp.sum(grad_probs * attn_probs, axis=-1, keepdims=True)
    )
    scores_low = grad_scores.astype(jnp.bfloat16)
    grad_query = (
        jnp.einsum(
            "bhqk,bkhd->bqhd",
            scores_low,
            split_heads(key_rows, item_count),
            preferred_element_type=jnp.float32,
        )
        * score_scale
    )
    grad_keys = (
        jnp.einsum(
            "bhqk,bqhd->bkhd",
            scores_low,
            split_heads(queries, item_count),
            preferred_element_type=jnp.float32,
        )
        * score_scale
    )
    return (
        merge_heads(grad_query).astype(jnp.bfloat16),
        merge_heads(grad_keys).astype(jnp.bfloat16),
        merge_heads(grad_values).astype(jnp.bfloat16),
    )


def projection_grads(source_q, source_kv, weights, grad_set):
    grad_query, grad_keys, grad_values = grad_set
    w_grads = [
        weight_grad(source_q, grad_query),
        weight_grad(source_kv, grad_keys),
        weight_grad(source_kv, grad_values),
    ]
    b_grads = jnp.stack([column_sum(grad_query), column_sum(grad_values)])
    back_query = linear_back(grad_query, weights[0])
    back_kv = linear_back(grad_keys, weights[1]) + linear_back(grad_values, weights[2])
    return (w_grads, b_grads, back_query, back_kv)


def gather_rows(former, latter):
    return (
        lax.all_gather(former, "tensor", axis=0, tiled=True),
        lax.all_gather(latter, "tensor", axis=0, tiled=True),
    )


def scatter_rows(former, latter):
    return (
        lax.psum_scatter(
            former.astype(jnp.bfloat16), "tensor", scatter_dimension=0, tiled=True
        ).astype(jnp.float32),
        lax.psum_scatter(
            latter.astype(jnp.bfloat16), "tensor", scatter_dimension=0, tiled=True
        ).astype(jnp.float32),
    )


def gather_grads(former, latter):
    return (
        lax.all_gather(former, "tensor", axis=0, tiled=True),
        lax.all_gather(latter, "tensor", axis=0, tiled=True),
    )


def scatter_grads(former, latter):
    return (
        lax.psum_scatter(
            former.astype(jnp.bfloat16), "tensor", scatter_dimension=0, tiled=True
        ).astype(jnp.float32),
        lax.psum_scatter(
            latter.astype(jnp.bfloat16), "tensor", scatter_dimension=0, tiled=True
        ).astype(jnp.float32),
    )


def flipped_grad(source, upstream):
    return weight_grad(upstream, source)


def share_sum(grads):
    joined = jnp.concatenate([g.astype(jnp.bfloat16) for g in grads], axis=1)
    return lax.psum_scatter(joined, "dp", scatter_dimension=0, tiled=True)


def small_sum_kernel(n_dp, n_tensor, wide, x_ref, o_ref, held, landed, send_sem, recv_sem):
    dp = lax.axis_index("dp")
    tensor = lax.axis_index("tensor")
    hops = []
    bit = 1
    while bit < n_tensor:
        hops.append((False, bit))
        bit *= 2
    bit = 1
    while bit < n_dp:
        hops.append((True, bit))
        bit *= 2

    def flip(index, bit):
        return index + bit - 2 * bit * lax.rem(index // bit, 2)

    def partner(along_dp, bit):
        return (flip(dp, bit), tensor) if along_dp else (dp, flip(tensor, bit))

    barrier = pltpu.get_barrier_semaphore()
    for hop in hops:
        pl.semaphore_signal(
            barrier, inc=1, device_id=partner(*hop), device_id_type=pl.DeviceIdType.MESH
        )
    pl.semaphore_wait(barrier, len(hops))
    held[0] = x_ref[...]
    for step, hop in enumerate(hops):
        rows = x_ref.shape[0] if hop[0] else wide
        copy = pltpu.make_async_remote_copy(
            src_ref=held.at[step, pl.ds(0, rows)],
            dst_ref=landed.at[step, pl.ds(0, rows)],
            send_sem=send_sem.at[step],
            recv_sem=recv_sem.at[step],
            device_id=partner(*hop),
            device_id_type=pl.DeviceIdType.MESH,
        )
        copy.start()
        copy.wait()
        if rows < x_ref.shape[0]:
            held[step + 1, pl.ds(0, rows)] = (
                held[step, pl.ds(0, rows)] + landed[step, pl.ds(0, rows)]
            )
            held[step + 1, pl.ds(rows, x_ref.shape[0] - rows)] = held[
                step, pl.ds(rows, x_ref.shape[0] - rows)
            ]
        else:
            held[step + 1] = held[step] + landed[step]
    o_ref[...] = held[len(hops)]


def small_sum(stacked, wide):
    n_dp, n_tensor = lax.axis_size("dp"), lax.axis_size("tensor")
    steps = n_dp.bit_length() + n_tensor.bit_length() - 2
    vmem = pl.BlockSpec(memory_space=pltpu.VMEM)
    return pl.pallas_call(
        functools.partial(small_sum_kernel, n_dp, n_tensor, wide),
        out_shape=jax.ShapeDtypeStruct(stacked.shape, jnp.float32),
        in_specs=[vmem],
        out_specs=vmem,
        scratch_shapes=[
            pltpu.VMEM((steps + 1,) + stacked.shape, jnp.float32),
            pltpu.VMEM((steps,) + stacked.shape, jnp.float32),
            pltpu.SemaphoreType.DMA((steps,)),
            pltpu.SemaphoreType.DMA((steps,)),
        ],
        compiler_params=pltpu.CompilerParams(collective_id=0, has_side_effects=True),
        name="small_sum",
    )(stacked)


def body(
    lang_in,
    visn_in,
    word_mask,
    task_flag,
    group_id,
    task_table,
    group_table,
    attn_in,
    attn_qv_bias,
    attn_out,
    ffn_in,
    ffn_in_bias,
    ffn_out,
    out_bias,
    norm_gain,
    norm_bias,
    lang_cot,
    visn_cot,
):
    item_count = word_mask.shape[0]
    lang_rows = lang_in.shape[0]
    visn_rows = visn_in.shape[0]
    tensor_place = lax.axis_index("tensor")
    item_ids = jnp.arange(item_count, dtype=jnp.int32)
    lang_item = (tensor_place * lang_rows + jnp.arange(lang_rows, dtype=jnp.int32)) // WORDS
    visn_item = (tensor_place * visn_rows + jnp.arange(visn_rows, dtype=jnp.int32)) // REGIONS
    lang_pick = (lang_item[:, None] == item_ids[None, :]).astype(jnp.bfloat16)
    visn_pick = (visn_item[:, None] == item_ids[None, :]).astype(jnp.bfloat16)
    task_pick = (task_flag[:, None] == jnp.arange(TASKS, dtype=jnp.int32)[None, :]).astype(
        jnp.bfloat16
    )
    group_pick = (group_id[:, None] == jnp.arange(GROUPS, dtype=jnp.int32)[None, :]).astype(
        jnp.bfloat16
    )
    lang_task = linear(lang_pick, task_pick)
    visn_group = linear(visn_pick, group_pick)
    lang_base = lang_in.astype(jnp.float32) + linear(lang_task.astype(jnp.bfloat16), task_table)
    visn_base = visn_in.astype(jnp.float32) + linear(visn_group.astype(jnp.bfloat16), group_table)
    gains = norm_gain.astype(jnp.float32)
    shifts = norm_bias.astype(jnp.float32)
    offsets = out_bias.astype(jnp.float32)
    qv_bias = attn_qv_bias.astype(jnp.float32)
    hidden_bias = ffn_in_bias.astype(jnp.float32)
    keep_words = word_mask > 0
    lang_low = lang_base.astype(jnp.bfloat16)
    visn_low = visn_base.astype(jnp.bfloat16)
    lang_all, visn_all = gather_rows(lang_low, visn_low)
    cross_lang, saved_cross_lang = attend_forward(
        lang_all, visn_all, None, attn_in[0], qv_bias[0], item_count
    )
    cross_visn, saved_cross_visn = attend_forward(
        visn_all, lang_all, keep_words, attn_in[0], qv_bias[0], item_count
    )
    part_lang, part_visn = scatter_rows(
        linear(cross_lang, attn_out[0]), linear(cross_visn, attn_out[0])
    )
    lang_one, stash_l0 = norm_forward(lang_base + part_lang + offsets[0], gains[0], shifts[0])
    visn_one, stash_v0 = norm_forward(visn_base + part_visn + offsets[0], gains[0], shifts[0])
    self_lang, self_visn = gather_rows(lang_one.astype(jnp.bfloat16), visn_one.astype(jnp.bfloat16))
    ctx_lang, saved_lang = attend_forward(
        self_lang, self_lang, keep_words, attn_in[1], qv_bias[1], item_count
    )
    ctx_visn, saved_visn = attend_forward(
        self_visn, self_visn, None, attn_in[2], qv_bias[2], item_count
    )
    part_lang, part_visn = scatter_rows(
        linear(ctx_lang, attn_out[1]), linear(ctx_visn, attn_out[2])
    )
    lang_two, stash_l1 = norm_forward(lang_one + part_lang + offsets[1], gains[1], shifts[1])
    visn_two, stash_v2 = norm_forward(visn_one + part_visn + offsets[2], gains[2], shifts[2])
    ffn_lang, ffn_visn = gather_rows(lang_two.astype(jnp.bfloat16), visn_two.astype(jnp.bfloat16))
    pre_lang = linear(ffn_lang, ffn_in[0]) + hidden_bias[0]
    pre_visn = linear(ffn_visn, ffn_in[1]) + hidden_bias[1]
    act_lang = gelu_value(pre_lang).astype(jnp.bfloat16)
    act_visn = gelu_value(pre_visn).astype(jnp.bfloat16)
    part_lang, part_visn = scatter_rows(linear(act_lang, ffn_out[0]), linear(act_visn, ffn_out[1]))
    lang_out, stash_l3 = norm_forward(lang_two + part_lang + offsets[3], gains[3], shifts[3])
    visn_out, stash_v4 = norm_forward(visn_two + part_visn + offsets[4], gains[4], shifts[4])
    top_lang, gain_l3, shift_l3, offset_l3 = norm_backward(
        lang_cot.astype(jnp.float32), stash_l3, gains[3]
    )
    top_visn, gain_v4, shift_v4, offset_v4 = norm_backward(
        visn_cot.astype(jnp.float32), stash_v4, gains[4]
    )
    down_lang, down_visn = gather_grads(
        top_lang.astype(jnp.bfloat16), top_visn.astype(jnp.bfloat16)
    )
    inner_lang = (linear_back(down_lang, ffn_out[0]) * gelu_slope(pre_lang)).astype(jnp.bfloat16)
    inner_visn = (linear_back(down_visn, ffn_out[1]) * gelu_slope(pre_visn)).astype(jnp.bfloat16)
    ffn_share = share_sum(
        [
            weight_grad(ffn_lang, inner_lang),
            weight_grad(ffn_visn, inner_visn),
            flipped_grad(act_lang, down_lang),
            flipped_grad(act_visn, down_visn),
        ]
    )
    ffn_bias_grads = jnp.stack([column_sum(inner_lang), column_sum(inner_visn)])
    back_lang, back_visn = scatter_grads(
        linear_back(inner_lang, ffn_in[0]), linear_back(inner_visn, ffn_in[1])
    )
    grad_two_lang = top_lang + back_lang
    grad_two_visn = top_visn + back_visn
    top_lang, gain_l1, shift_l1, offset_l1 = norm_backward(grad_two_lang, stash_l1, gains[1])
    top_visn, gain_v2, shift_v2, offset_v2 = norm_backward(grad_two_visn, stash_v2, gains[2])
    mid_lang, mid_visn = gather_grads(top_lang.astype(jnp.bfloat16), top_visn.astype(jnp.bfloat16))
    out_grad_lang = flipped_grad(ctx_lang, mid_lang)
    out_grad_visn = flipped_grad(ctx_visn, mid_visn)
    grads_lang = attend_backward(linear_back(mid_lang, attn_out[1]), saved_lang, item_count)
    grads_visn = attend_backward(linear_back(mid_visn, attn_out[2]), saved_visn, item_count)
    win_lang, bias_lang, query_lang, kv_lang = projection_grads(
        self_lang, self_lang, attn_in[1], grads_lang
    )
    win_visn, bias_visn, query_visn, kv_visn = projection_grads(
        self_visn, self_visn, attn_in[2], grads_visn
    )
    self_share = share_sum(win_lang + win_visn + [out_grad_lang, out_grad_visn])
    back_lang, back_visn = scatter_grads(query_lang + kv_lang, query_visn + kv_visn)
    grad_one_lang = top_lang + back_lang
    grad_one_visn = top_visn + back_visn
    top_lang, gain_l0, shift_l0, offset_l0 = norm_backward(grad_one_lang, stash_l0, gains[0])
    top_visn, gain_v0, shift_v0, offset_v0 = norm_backward(grad_one_visn, stash_v0, gains[0])
    cross_dlang, cross_dvisn = gather_grads(
        top_lang.astype(jnp.bfloat16), top_visn.astype(jnp.bfloat16)
    )
    cross_out_grad = flipped_grad(cross_lang, cross_dlang) + flipped_grad(cross_visn, cross_dvisn)
    grads_cross_lang = attend_backward(
        linear_back(cross_dlang, attn_out[0]), saved_cross_lang, item_count
    )
    grads_cross_visn = attend_backward(
        linear_back(cross_dvisn, attn_out[0]), saved_cross_visn, item_count
    )
    win_first, bias_first, query_from_lang, kv_from_visn = projection_grads(
        lang_all, visn_all, attn_in[0], grads_cross_lang
    )
    win_second, bias_second, query_from_visn, kv_from_lang = projection_grads(
        visn_all, lang_all, attn_in[0], grads_cross_visn
    )
    cross_share = share_sum(
        [first + second for first, second in zip(win_first, win_second)] + [cross_out_grad]
    )
    back_lang, back_visn = scatter_grads(
        query_from_lang + kv_from_lang, query_from_visn + kv_from_visn
    )
    base_grad_lang = top_lang + back_lang
    base_grad_visn = top_visn + back_visn
    qv_grads = jnp.stack([bias_first + bias_second, bias_lang, bias_visn])
    offset_part = jnp.stack([offset_l0 + offset_v0, offset_l1, offset_v2, offset_l3, offset_v4])
    gain_part = jnp.stack([gain_l0 + gain_v0, gain_l1, gain_v2, gain_l3, gain_v4])
    shift_part = jnp.stack([shift_l0 + shift_v0, shift_l1, shift_v2, shift_l3, shift_v4])
    task_part = lax.dot_general(
        lang_task,
        base_grad_lang,
        (((0,), (0,)), ((), ())),
        precision=highest,
        preferred_element_type=jnp.float32,
    )
    group_part = lax.dot_general(
        visn_group,
        base_grad_visn,
        (((0,), (0,)), ((), ())),
        precision=highest,
        preferred_element_type=jnp.float32,
    )
    head_cols = attn_in.shape[3]
    hidden_cols = ffn_in.shape[2]
    share_rows = cross_share.shape[0]
    cross_parts = cross_share.astype(jnp.float32).reshape(share_rows, 4, head_cols)
    self_parts = self_share.astype(jnp.float32).reshape(share_rows, 8, head_cols)
    ffn_parts = ffn_share.astype(jnp.float32).reshape(share_rows, 4, hidden_cols)
    attn_in_grads = jnp.stack(
        [
            cross_parts[:, 0:3].transpose(1, 0, 2),
            self_parts[:, 0:3].transpose(1, 0, 2),
            self_parts[:, 3:6].transpose(1, 0, 2),
        ]
    )
    attn_out_grads = jnp.stack([cross_parts[:, 3].T, self_parts[:, 6].T, self_parts[:, 7].T])
    ffn_in_grads = ffn_parts[:, 0:2].transpose(1, 0, 2)
    ffn_out_grads = ffn_parts[:, 2:4].transpose(1, 2, 0)
    width = task_part.shape[1]
    wide_rows = jnp.concatenate(
        [task_part, group_part, offset_part, gain_part, shift_part, jnp.zeros((1, width))]
    )
    bias_rows = jnp.concatenate(
        [ffn_bias_grads, jnp.pad(qv_grads.reshape(6, head_cols), ((0, 0), (0, width - head_cols)))]
    )
    summed = small_sum(jnp.concatenate([wide_rows, bias_rows]), wide_rows.shape[0])
    task_grad, group_grad = summed[0:3], summed[3:8]
    offset_grad, gain_grad, shift_grad = summed[8:13], summed[13:18], summed[18:23]
    ffn_bias_grads = summed[24:26]
    qv_grads = summed[26:32, :head_cols].reshape(3, 2, head_cols)
    return (
        lang_out.astype(jnp.bfloat16),
        visn_out.astype(jnp.bfloat16),
        base_grad_lang.astype(jnp.bfloat16),
        base_grad_visn.astype(jnp.bfloat16),
        task_grad,
        group_grad,
        attn_in_grads,
        qv_grads,
        attn_out_grads,
        ffn_in_grads,
        ffn_bias_grads,
        ffn_out_grads,
        offset_grad,
        gain_grad,
        shift_grad,
    )


def solution(mesh):
    placed = (
        P(("dp", "tensor"), None),
        P(("dp", "tensor"), None),
        P("dp", None),
        P("dp"),
        P("dp"),
        P(),
        P(),
        P(None, None, None, "tensor"),
        P(None, None, "tensor"),
        P(None, "tensor", None),
        P(None, None, "tensor"),
        P(None, "tensor"),
        P(None, "tensor", None),
        P(),
        P(),
        P(),
        P(("dp", "tensor"), None),
        P(("dp", "tensor"), None),
    )
    return jax.shard_map(
        body,
        mesh=mesh,
        in_specs=placed,
        out_specs=(
            P(("dp", "tensor"), None),
            P(("dp", "tensor"), None),
            P(("dp", "tensor"), None),
            P(("dp", "tensor"), None),
            P(),
            P(),
            P(None, None, "dp", "tensor"),
            P(None, None, "tensor"),
            P(None, "tensor", "dp"),
            P(None, "dp", "tensor"),
            P(None, "tensor"),
            P(None, "tensor", "dp"),
            P(),
            P(),
            P(),
        ),
        check_vma=False,
    )
```
